32 devices in a mesh: dom: 16 (over z, y, x), st: 2 (over core).
Axes of the slice: x: 2, y: 2, z: 4, core: 2. Of those that a mesh axis runs over, the one named last changes fastest.
Arguments:
- psi: float32 [2, 16, 8, 2, 64, 256], P(None, 'dom', None, None, None, 'st'), parts along dimension 5, may hold values from -18 to 18
- potential: float32 [16, 8, 2, 64], P('dom'), may hold values from 0 to 4
Outputs:
- propagated: float32 [2, 16, 8, 2, 64, 256], P(None, 'dom', None, None, None, 'st'), parts along dimension 5
The draws below stay inside these ranges and needn't reach their ends.
There are 2 independent parts, one for each index of `st`. The reference program is written for one: setup_inputs(seed, part) draws one part's arguments, and reference() takes and returns one part's arrays. A program takes and returns all parts, laid end to end along the dimension named above; an argument that names none is the same for every part. Nothing has to cross between parts.
All inputs are finite; a program needn't handle non-finite values.
Results may differ from the reference program's by a relative error of at most 0.0003.
Values sent between devices are 32-bit elements; how exact they have to be, the bound alone decides.
A program may use at most 128 MiB of HBM per device.

```python
import jax
import jax.numpy as jnp
from jax import lax

CX = 8
BY = 2
NZ = 64
ORB = 128
ITERS = 6
BLOCKS = 16


def draw_psi(key, part):
    shape = (2, BLOCKS, CX, BY, NZ, ORB)
    rising = 1.0 + 2.0 * jnp.arange(BLOCKS, dtype=jnp.float32) / max(BLOCKS - 1, 1)
    rising = rising.reshape(1, BLOCKS, 1, 1, 1, 1)
    return jnp.clip(jax.random.normal(key, shape, jnp.float32), -6.0, 6.0) * rising


def steps_of(rng, dims, shards, smallest, high):
    loudness = 1.0
    for dim, shards_of in shards:
        heights = jax.random.uniform(jax.random.fold_in(jax.random.fold_in(rng, 6), dim), (shards_of,), jnp.float32, smallest / len(shards), high / len(shards))
        loudness = loudness * jnp.repeat(jnp.exp(heights), dims[dim] // shards_of).reshape((-1,) + (1,) * (len(dims) - 1 - dim))
    return loudness


def setup_inputs(seed: int = 0, part: int = 0) -> dict:
    keys = jax.random.split(jax.random.key(seed), 3)
    part_keys = jax.random.split(jax.random.fold_in(keys[2], part), 3)
    psi = draw_psi(jax.random.fold_in(jax.random.fold_in(keys[2], part), 71), part)
    potential = jnp.clip(4.0 * jax.random.uniform(keys[1], (BLOCKS, CX, BY, NZ), jnp.float32) ** steps_of(keys[1], (BLOCKS, CX, BY, NZ), ((0, 16),), -0.2, 0.2), 0.0, 4.0)
    return dict(psi=psi, potential=potential)


epsilon = 1e-06
time_step = 0.5
taylor_terms = 32
far_weight = -1.0 / 12.0
near_weight = 4.0 / 3.0
centre_weight = -7.5

def to_grid(blocked):
    parts, nblocks, cx, by, nz, orbs = blocked.shape
    grid = blocked.transpose(0, 2, 1, 3, 4, 5)
    return grid.reshape(parts, cx, nblocks * by, nz, orbs)

def to_blocks(grid, by):
    parts, nx, ny, nz, orbs = grid.shape
    blocked = grid.reshape(parts, nx, ny // by, by, nz, orbs).transpose(0, 2, 1, 3, 4, 5)
    return blocked

def shift_walls(values, offset):
    width_y = values.shape[2]
    padded = jnp.pad(values, ((0, 0), (0, 0), (2, 2), (0, 0), (0, 0)))
    return padded[:, :, 2 - offset:2 - offset + width_y]

def hamiltonian(values_in, potential):
    total = centre_weight * values_in
    for along in (1, 3):
        total = total + near_weight * (jnp.roll(values_in, 1, along) + jnp.roll(values_in, -1, along))
        total = total + far_weight * (jnp.roll(values_in, 2, along) + jnp.roll(values_in, -2, along))
    total = total + near_weight * (shift_walls(values_in, 1) + shift_walls(values_in, -1))
    total = total + far_weight * (shift_walls(values_in, 2) + shift_walls(values_in, -2))
    return -0.5 * total + potential[None, :, :, :, None] * values_in

def tridiagonal(alphas, betas, vector):
    zero_row = jnp.zeros((1, vector.shape[1]), jnp.float32)
    upper = jnp.concatenate([betas * vector[1:], zero_row], axis=0)
    lower = jnp.concatenate([zero_row, betas * vector[:-1]], axis=0)
    return alphas * vector + upper + lower

def krylov_exponential(alphas, betas):
    count = alphas.shape[0]
    first = (jnp.arange(count) == 0).astype(jnp.float32)[:, None] * jnp.ones_like(alphas)
    term_real = first
    term_imag = jnp.zeros_like(alphas)
    sum_real = term_real
    sum_imag = term_imag
    for order in range(1, taylor_terms):
        applied_real = tridiagonal(alphas, betas, term_real)
        applied_imag = tridiagonal(alphas, betas, term_imag)
        term_real = time_step * applied_imag / order
        term_imag = -time_step * applied_real / order
        sum_real = sum_real + term_real
        sum_imag = sum_imag + term_imag
    return (sum_real, sum_imag)

def reference(psi, potential):
    by = psi.shape[3]
    grid_psi = to_grid(psi)
    grid_pot = to_grid(potential[None, :, :, :, :, None])[0, :, :, :, 0]
    axes_all = (0, 1, 2, 3)
    first_norm = jnp.sqrt(lax.optimization_barrier(jnp.sum(grid_psi * grid_psi, axis=axes_all)) + epsilon)
    vector = grid_psi / first_norm
    previous = jnp.zeros_like(vector)
    beta_prev = jnp.zeros_like(first_norm)
    krylov_basis = []
    alpha_list = []
    beta_list = []
    for iteration in range(ITERS):
        applied = hamiltonian(vector, grid_pot)
        alpha_now = lax.optimization_barrier(jnp.sum(vector * applied, axis=axes_all))
        krylov_basis.append(vector)
        alpha_list.append(alpha_now)
        if iteration + 1 < ITERS:
            remainder = applied - alpha_now * vector - beta_prev * previous
            beta_now = jnp.sqrt(lax.optimization_barrier(jnp.sum(remainder * remainder, axis=axes_all)) + epsilon)
            previous = vector
            vector = remainder / beta_now
            beta_prev = beta_now
            beta_list.append(beta_now)
    coef_real, coef_imag = krylov_exponential(jnp.stack(alpha_list), jnp.stack(beta_list))
    out_real = jnp.zeros_like(grid_psi[0])
    out_imag = jnp.zeros_like(grid_psi[0])
    for index_j in range(ITERS):
        basis_now = krylov_basis[index_j]
        out_real = out_real + coef_real[index_j] * basis_now[0] - coef_imag[index_j] * basis_now[1]
        out_imag = out_imag + coef_real[index_j] * basis_now[1] + coef_imag[index_j] * basis_now[0]
    return to_blocks(first_norm * jnp.stack([out_real, out_imag]), by)
```

```python
import functools

import jax
import jax.numpy as jnp
from jax import lax
from jax.experimental import pallas as pl
from jax.experimental.pallas import tpu as pltpu
from jax.sharding import PartitionSpec as P

ITERS = 6


epsilon = 1e-06
time_step = 0.5
taylor_terms = 32
far_weight = -1.0 / 12.0
near_weight = 4.0 / 3.0
centre_weight = -7.5


def to_grid(blocked):
    parts, nblocks, cx, by, nz, orbs = blocked.shape
    grid = blocked.transpose(0, 2, 1, 3, 4, 5)
    return grid.reshape(parts, cx, nblocks * by, nz, orbs)


def to_blocks(grid, by):
    parts, nx, ny, nz, orbs = grid.shape
    blocked = grid.reshape(parts, nx, ny // by, by, nz, orbs).transpose(0, 2, 1, 3, 4, 5)
    return blocked


def shift_walls(values, offset):
    width_y = values.shape[2]
    padded = jnp.pad(values, ((0, 0), (0, 0), (2, 2), (0, 0), (0, 0)))
    return padded[:, :, 2 - offset : 2 - offset + width_y]


def hamiltonian_whole(values_in, potential):
    total = centre_weight * values_in
    for along in (1, 3):
        total = total + near_weight * (
            jnp.roll(values_in, 1, along) + jnp.roll(values_in, -1, along)
        )
        total = total + far_weight * (
            jnp.roll(values_in, 2, along) + jnp.roll(values_in, -2, along)
        )
    total = total + near_weight * (shift_walls(values_in, 1) + shift_walls(values_in, -1))
    total = total + far_weight * (shift_walls(values_in, 2) + shift_walls(values_in, -2))
    return -0.5 * total + potential[None, :, :, :, None] * values_in


def tridiagonal(alphas, betas, vector):
    zero_row = jnp.zeros((1, vector.shape[1]), jnp.float32)
    upper = jnp.concatenate([betas * vector[1:], zero_row], axis=0)
    lower = jnp.concatenate([zero_row, betas * vector[:-1]], axis=0)
    return alphas * vector + upper + lower


def krylov_exponential(alphas, betas):
    count = alphas.shape[0]
    first = (jnp.arange(count) == 0).astype(jnp.float32)[:, None] * jnp.ones_like(alphas)
    term_real = first
    term_imag = jnp.zeros_like(alphas)
    sum_real = term_real
    sum_imag = term_imag
    for order in range(1, taylor_terms):
        applied_real = tridiagonal(alphas, betas, term_real)
        applied_imag = tridiagonal(alphas, betas, term_imag)
        term_real = time_step * applied_imag / order
        term_imag = -time_step * applied_real / order
        sum_real = sum_real + term_real
        sum_imag = sum_imag + term_imag
    return (sum_real, sum_imag)


def combine_basis(krylov_basis, alpha_list, beta_list, first_norm):
    coef_real, coef_imag = krylov_exponential(jnp.stack(alpha_list), jnp.stack(beta_list))
    out_real = jnp.zeros_like(krylov_basis[0][0])
    out_imag = jnp.zeros_like(krylov_basis[0][0])
    for index_j in range(len(krylov_basis)):
        basis_now = krylov_basis[index_j]
        out_real = out_real + coef_real[index_j] * basis_now[0] - coef_imag[index_j] * basis_now[1]
        out_imag = out_imag + coef_real[index_j] * basis_now[1] + coef_imag[index_j] * basis_now[0]
    return first_norm * jnp.stack([out_real, out_imag])


def local_lanczos(grid_psi, grid_pot):
    axes_all = (0, 1, 2, 3)
    first_norm = jnp.sqrt(jnp.sum(grid_psi * grid_psi, axis=axes_all) + epsilon)
    vector = grid_psi / first_norm
    previous = jnp.zeros_like(vector)
    beta_prev = jnp.zeros_like(first_norm)
    krylov_basis = []
    alpha_list = []
    beta_list = []
    for iteration in range(ITERS):
        applied = hamiltonian_whole(vector, grid_pot)
        alpha_now = jnp.sum(vector * applied, axis=axes_all)
        krylov_basis.append(vector)
        alpha_list.append(alpha_now)
        if iteration + 1 < ITERS:
            remainder = applied - alpha_now * vector - beta_prev * previous
            beta_now = jnp.sqrt(jnp.sum(remainder * remainder, axis=axes_all) + epsilon)
            previous = vector
            vector = remainder / beta_now
            beta_prev = beta_now
            beta_list.append(beta_now)
    return combine_basis(krylov_basis, alpha_list, beta_list, first_norm)


def on_device(psi, potential):
    by = psi.shape[3]
    moved = lax.all_to_all(psi, "dom", split_axis=5, concat_axis=1, tiled=True)
    whole_pot = lax.all_gather(potential, "dom", axis=0, tiled=True)
    grid_pot = to_grid(whole_pot[None, :, :, :, :, None])[0, :, :, :, 0]
    result = to_blocks(local_lanczos(to_grid(moved), grid_pot), by)
    return lax.all_to_all(result, "dom", split_axis=1, concat_axis=5, tiled=True)


SUB = 8
LANES = 128
HALF = SUB // 2
CHUNKS = 2
UNROLL_A = 2
UNROLL_B = 2


def swap_parts(x):
    return pltpu.roll(x, HALF, 0)


def total_of(acc):
    summed = jnp.broadcast_to(jnp.sum(acc, axis=1, keepdims=True), (SUB, LANES))
    return summed + swap_parts(summed)


def krylov_weights(alphas, betas):
    count = len(alphas)
    one = jnp.ones((SUB, LANES), jnp.float32)
    term = [one] + [None] * (count - 1)
    real = [one] + [None] * (count - 1)
    imag = [None] * count
    for order in range(1, taylor_terms):
        fresh = []
        for i in range(count):
            pieces = []
            if term[i] is not None:
                pieces.append(alphas[i] * term[i])
            if i + 1 < count and term[i + 1] is not None:
                pieces.append(betas[i] * term[i + 1])
            if i > 0 and term[i - 1] is not None:
                pieces.append(betas[i - 1] * term[i - 1])
            fresh.append(sum(pieces[1:], pieces[0]) * (time_step / order) if pieces else None)
        term = fresh
        into = imag if order % 2 else real
        minus = order % 4 in (1, 2)
        for i in range(count):
            if term[i] is not None:
                if into[i] is None:
                    into[i] = -term[i] if minus else term[i]
                else:
                    into[i] = into[i] - term[i] if minus else into[i] + term[i]
    zero = jnp.zeros((SUB, LANES), jnp.float32)
    return [zero if r is None else r for r in real], [zero if m is None else m for m in imag]


def kernel(n, nx, nz, psi_ref, pot_ref, out_ref, send, recv, basis, outb, back, pots,
           send_sem, recv_sem, pot_send, pot_recv, back_send, back_recv):
    me = lax.axis_index("dom")
    mesh_ids = pl.DeviceIdType.MESH
    barrier = pltpu.get_barrier_semaphore()

    def greet(k, carry):
        pl.semaphore_signal(barrier, inc=1, device_id={"dom": lax.rem(me + k, n)}, device_id_type=mesh_ids)
        return carry

    lax.fori_loop(1, n, greet, 0)

    def forward(c, here, there):
        return pltpu.make_async_remote_copy(
            src_ref=send.at[c, there], dst_ref=recv.at[c, here + 1],
            send_sem=send_sem.at[c, there], recv_sem=recv_sem.at[c, here],
            device_id={"dom": there}, device_id_type=mesh_ids)

    def pot_copy(here, there):
        return pltpu.make_async_remote_copy(
            src_ref=pot_ref, dst_ref=pots.at[here],
            send_sem=pot_send.at[there], recv_sem=pot_recv.at[here],
            device_id={"dom": there}, device_id_type=mesh_ids)

    def backward(c, here, there):
        return pltpu.make_async_remote_copy(
            src_ref=outb.at[c, there], dst_ref=back.at[c, here],
            send_sem=back_send.at[c, there], recv_sem=back_recv.at[c, here],
            device_id={"dom": there}, device_id_type=mesh_ids)

    low = lax.broadcasted_iota(jnp.int32, (n, SUB, LANES), 1) < HALF

    def interleave(a, b):
        return (jnp.where(low, a, pltpu.roll(b, HALF, 1)), jnp.where(low, pltpu.roll(a, HALF, 1), b))

    def pack(x, carry):
        parts = [psi_ref[p * nx + x].T.reshape(n, SUB, LANES) for p in range(2)]
        for c, block in enumerate(interleave(*parts)):
            send[c, :, x] = block
        return carry

    lax.fori_loop(0, nx, pack, 0)

    pots[me] = pot_ref[...]
    blank = jnp.zeros((nx, SUB, LANES), jnp.float32)
    for c in range(CHUNKS):
        recv[c, me + 1] = send[c, me]
        recv[c, 0] = blank
        recv[c, n + 1] = blank
    for j in range(ITERS - 1):
        basis[j, 0] = blank
        basis[j, n + 1] = blank

    pl.semaphore_wait(barrier, n - 1)

    def send_pot(k, carry):
        pot_copy(me, lax.rem(me + k, n)).start()
        return carry

    lax.fori_loop(1, n, send_pot, 0)
    for c in range(CHUNKS):
        def send_one(k, carry, c=c):
            forward(c, me, lax.rem(me + k, n)).start()
            return carry

        lax.fori_loop(1, n, send_one, 0)

    def wait_pot(k, carry):
        there = lax.rem(me + n - k, n)
        pot_copy(there, there).wait_recv()
        return carry

    lane = lax.broadcasted_iota(jnp.int32, (SUB, LANES), 1)
    upper = lane >= nz
    cell = lax.rem(lane, nz)
    sign = jnp.where(lax.broadcasted_iota(jnp.int32, (SUB, LANES), 0) < HALF, 1.0, -1.0)
    masks = {1: cell < 1, 2: cell < 2, -1: cell >= nz - 1, -2: cell >= nz - 2}
    near, far = -0.5 * near_weight, -0.5 * far_weight
    rotate = lambda u, by: pltpu.roll(u, by % LANES, 1)

    def along_z(u, by):
        return jnp.where(masks[by], rotate(u, by + nz), rotate(u, by))

    def applied_at(ref, s):
        before = [ref[s, x] for x in range(nx)]
        now = [ref[s + 1, x] for x in range(nx)]
        after = [ref[s + 2, x] for x in range(nx)]
        result = []
        for x in range(nx):
            u = now[x]
            close = now[(x + 1) % nx] + now[(x - 1) % nx]
            close = close + rotate(u + jnp.where(upper, before[x], after[x]), nz)
            close = close + along_z(u, 1) + along_z(u, -1)
            wide = now[(x + 2) % nx] + now[(x - 2) % nx] + before[x] + after[x]
            wide = wide + along_z(u, 2) + along_z(u, -2)
            own = jnp.broadcast_to(pots[s, pl.ds(x, 1), :], (SUB, LANES)) + -0.5 * centre_weight
            result.append(own * u + near * close + far * wide)
        return now, result

    def chunk(c, carry):
        vectors = [recv.at[c]] + [basis.at[j] for j in range(ITERS - 1)]

        def arrive(k, acc):
            there = lax.rem(me + n - k, n)
            forward(c, there, there).wait_recv()
            for x in range(nx):
                u = recv[c, there + 1, x]
                acc = acc + u * u
            return acc

        acc = jnp.zeros((SUB, LANES), jnp.float32)
        for x in range(nx):
            u = recv[c, me + 1, x]
            acc = acc + u * u
        acc = lax.fori_loop(1, n, arrive, acc)
        first_norm = jnp.sqrt(total_of(acc) + epsilon)

        @pl.when(c == 0)
        def _():
            lax.fori_loop(1, n, wait_pot, 0)

        scales = [1.0 / first_norm]
        alphas, betas = [], []
        zero = jnp.zeros((SUB, LANES), jnp.float32)
        for j in range(ITERS):
            ref = vectors[j]
            last = j + 1 == ITERS
            fresh = None if last else vectors[j + 1]

            def apply(s, accs, ref=ref, fresh=fresh):
                accs = list(accs)
                now, result = applied_at(ref, s)
                for x in range(nx):
                    if fresh is not None:
                        fresh[s + 1, x] = result[x]
                    accs[x % 2] = accs[x % 2] + now[x] * result[x]
                return tuple(accs)

            accs = lax.fori_loop(0, n, apply, (zero, zero), unroll=UNROLL_A)
            scale = scales[j]
            alpha = scale * (scale * total_of(accs[0] + accs[1]))
            alphas.append(alpha)
            if last:
                break
            by_self = alpha * scale
            by_previous = betas[j - 1] * scales[j - 1] if j else None

            def reduce(s, accs, ref=ref, fresh=fresh, scale=scale, by_self=by_self, by_previous=by_previous, j=j):
                accs = list(accs)
                for x in range(nx):
                    r = scale * fresh[s + 1, x] - by_self * ref[s + 1, x]
                    if j:
                        r = r - by_previous * vectors[j - 1][s + 1, x]
                    fresh[s + 1, x] = r
                    accs[x % 2] = accs[x % 2] + r * r
                return tuple(accs)

            accs = lax.fori_loop(0, n, reduce, (zero, zero), unroll=UNROLL_B)
            beta = jnp.sqrt(total_of(accs[0] + accs[1]) + epsilon)
            betas.append(beta)
            scales.append(1.0 / beta)

        real, imag = krylov_weights(alphas, betas)
        straight = [first_norm * scales[j] * real[j] for j in range(ITERS)]
        crossed = [first_norm * scales[j] * imag[j] * sign for j in range(ITERS)]

        def combined(d, x):
            us = [v[d + 1, x] for v in vectors]
            a = straight[0] * us[0]
            b = crossed[0] * us[0]
            for j in range(1, ITERS):
                a = a + straight[j] * us[j]
                b = b + crossed[j] * us[j]
            return a + swap_parts(b)

        def finish(k, carry):
            there = lax.rem(me + k, n)
            for x in range(nx):
                outb[c, there, x] = combined(there, x)

            @pl.when(k > 1)
            def _():
                backward(c, me, lax.rem(me + k - 1, n)).start()

            return carry

        lax.fori_loop(1, n, finish, 0)
        for x in range(nx):
            back[c, me, x] = combined(me, x)
        backward(c, me, lax.rem(me + n - 1, n)).start()
        return carry

    lax.fori_loop(0, CHUNKS, chunk, 0)

    for c in range(CHUNKS):
        def returned(k, carry, c=c):
            there = lax.rem(me + n - k, n)
            backward(c, there, there).wait_recv()
            return carry

        lax.fori_loop(1, n, returned, 0)

    def unpack(x, carry):
        for p, block in enumerate(interleave(back[0, :, x], back[1, :, x])):
            out_ref[p * nx + x] = block.reshape(n * SUB, LANES).T
        return carry

    lax.fori_loop(0, nx, unpack, 0)

    def sent(k, carry):
        there = lax.rem(me + k, n)
        pot_copy(me, there).wait_send()
        for c in range(CHUNKS):
            forward(c, me, there).wait_send()
            backward(c, me, there).wait_send()
        return carry

    lax.fori_loop(1, n, sent, 0)


def fused(psi, potential, n):
    parts, slabs, nx, by, nz, orbs = psi.shape
    rows = nx * by * nz // LANES
    vec = lambda *lead: pltpu.VMEM(lead + (nx, SUB, LANES), jnp.float32)
    dma = lambda *shape: pltpu.SemaphoreType.DMA(shape)
    result = pl.pallas_call(
        functools.partial(kernel, n, nx, nz),
        out_shape=jax.ShapeDtypeStruct((parts * nx, by * nz, orbs), jnp.float32),
        in_specs=[pl.BlockSpec(memory_space=pltpu.VMEM)] * 2,
        out_specs=pl.BlockSpec(memory_space=pltpu.VMEM),
        scratch_shapes=[
            vec(CHUNKS, n), vec(CHUNKS, n + 2), vec(ITERS - 1, n + 2), vec(CHUNKS, n), vec(CHUNKS, n),
            pltpu.VMEM((n, nx, LANES), jnp.float32),
            dma(CHUNKS, n), dma(CHUNKS, n), dma(n), dma(n), dma(CHUNKS, n), dma(CHUNKS, n),
        ],
        compiler_params=pltpu.CompilerParams(collective_id=0, has_side_effects=True),
    )(psi.reshape(parts * nx, by * nz, orbs), potential.reshape(nx, by * nz))
    return result.reshape(psi.shape)


def fits(psi, n):
    parts, slabs, nx, by, nz, orbs = psi.shape
    return parts == 2 and slabs == 1 and by == 2 and by * nz == LANES and orbs == LANES and orbs == n * SUB and n > 1


def per_device(n, psi, potential):
    if fits(psi, n):
        return fused(psi, potential, n)
    return on_device(psi, potential)


def solution(mesh):
    placed = (P(None, "dom", None, None, None, "st"), P("dom", None, None, None))
    return jax.shard_map(
        functools.partial(per_device, mesh.shape["dom"]),
        mesh=mesh,
        in_specs=placed,
        out_specs=P(None, "dom", None, None, None, "st"),
        check_vma=False,
    )
```

```python
import functools

import jax
import jax.numpy as jnp
from jax import lax
from jax.experimental import pallas as pl
from jax.experimental.pallas import tpu as pltpu
from jax.sharding import PartitionSpec as P

ITERS = 6


epsilon = 1e-06
time_step = 0.5
taylor_terms = 32
far_weight = -1.0 / 12.0
near_weight = 4.0 / 3.0
centre_weight = -7.5


def to_grid(blocked):
    parts, nblocks, cx, by, nz, orbs = blocked.shape
    grid = blocked.transpose(0, 2, 1, 3, 4, 5)
    return grid.reshape(parts, cx, nblocks * by, nz, orbs)


def to_blocks(grid, by):
    parts, nx, ny, nz, orbs = grid.shape
    blocked = grid.reshape(parts, nx, ny // by, by, nz, orbs).transpose(0, 2, 1, 3, 4, 5)
    return blocked


def shift_walls(values, offset):
    width_y = values.shape[2]
    padded = jnp.pad(values, ((0, 0), (0, 0), (2, 2), (0, 0), (0, 0)))
    return padded[:, :, 2 - offset : 2 - offset + width_y]


def hamiltonian_whole(values_in, potential):
    total = centre_weight * values_in
    for along in (1, 3):
        total = total + near_weight * (
            jnp.roll(values_in, 1, along) + jnp.roll(values_in, -1, along)
        )
        total = total + far_weight * (
            jnp.roll(values_in, 2, along) + jnp.roll(values_in, -2, along)
        )
    total = total + near_weight * (shift_walls(values_in, 1) + shift_walls(values_in, -1))
    total = total + far_weight * (shift_walls(values_in, 2) + shift_walls(values_in, -2))
    return -0.5 * total + potential[None, :, :, :, None] * values_in


def tridiagonal(alphas, betas, vector):
    zero_row = jnp.zeros((1, vector.shape[1]), jnp.float32)
    upper = jnp.concatenate([betas * vector[1:], zero_row], axis=0)
    lower = jnp.concatenate([zero_row, betas * vector[:-1]], axis=0)
    return alphas * vector + upper + lower


def krylov_exponential(alphas, betas):
    count = alphas.shape[0]
    first = (jnp.arange(count) == 0).astype(jnp.float32)[:, None] * jnp.ones_like(alphas)
    term_real = first
    term_imag = jnp.zeros_like(alphas)
    sum_real = term_real
    sum_imag = term_imag
    for order in range(1, taylor_terms):
        applied_real = tridiagonal(alphas, betas, term_real)
        applied_imag = tridiagonal(alphas, betas, term_imag)
        term_real = time_step * applied_imag / order
        term_imag = -time_step * applied_real / order
        sum_real = sum_real + term_real
        sum_imag = sum_imag + term_imag
    return (sum_real, sum_imag)


def combine_basis(krylov_basis, alpha_list, beta_list, first_norm):
    coef_real, coef_imag = krylov_exponential(jnp.stack(alpha_list), jnp.stack(beta_list))
    out_real = jnp.zeros_like(krylov_basis[0][0])
    out_imag = jnp.zeros_like(krylov_basis[0][0])
    for index_j in range(len(krylov_basis)):
        basis_now = krylov_basis[index_j]
        out_real = out_real + coef_real[index_j] * basis_now[0] - coef_imag[index_j] * basis_now[1]
        out_imag = out_imag + coef_real[index_j] * basis_now[1] + coef_imag[index_j] * basis_now[0]
    return first_norm * jnp.stack([out_real, out_imag])


def local_lanczos(grid_psi, grid_pot):
    axes_all = (0, 1, 2, 3)
    first_norm = jnp.sqrt(jnp.sum(grid_psi * grid_psi, axis=axes_all) + epsilon)
    vector = grid_psi / first_norm
    previous = jnp.zeros_like(vector)
    beta_prev = jnp.zeros_like(first_norm)
    krylov_basis = []
    alpha_list = []
    beta_list = []
    for iteration in range(ITERS):
        applied = hamiltonian_whole(vector, grid_pot)
        alpha_now = jnp.sum(vector * applied, axis=axes_all)
        krylov_basis.append(vector)
        alpha_list.append(alpha_now)
        if iteration + 1 < ITERS:
            remainder = applied - alpha_now * vector - beta_prev * previous
            beta_now = jnp.sqrt(jnp.sum(remainder * remainder, axis=axes_all) + epsilon)
            previous = vector
            vector = remainder / beta_now
            beta_prev = beta_now
            beta_list.append(beta_now)
    return combine_basis(krylov_basis, alpha_list, beta_list, first_norm)


def on_device(psi, potential):
    by = psi.shape[3]
    moved = lax.all_to_all(psi, "dom", split_axis=5, concat_axis=1, tiled=True)
    whole_pot = lax.all_gather(potential, "dom", axis=0, tiled=True)
    grid_pot = to_grid(whole_pot[None, :, :, :, :, None])[0, :, :, :, 0]
    result = to_blocks(local_lanczos(to_grid(moved), grid_pot), by)
    return lax.all_to_all(result, "dom", split_axis=1, concat_axis=5, tiled=True)


SUB = 8
LANES = 128
HALF = SUB // 2
CHUNKS = 2
GROUP = 4
UNROLL_A = 4
UNROLL_B = 8


def swap_parts(x):
    return pltpu.roll(x, HALF, 0)


def total_of(acc):
    summed = jnp.broadcast_to(jnp.sum(acc, axis=1, keepdims=True), (SUB, LANES))
    return summed + swap_parts(summed)


def krylov_weights(alphas, betas):
    count = len(alphas)
    one = jnp.ones((SUB, LANES), jnp.float32)
    term = [one] + [None] * (count - 1)
    real = [one] + [None] * (count - 1)
    imag = [None] * count
    for order in range(1, taylor_terms):
        fresh = []
        for i in range(count):
            pieces = []
            if term[i] is not None:
                pieces.append(alphas[i] * term[i])
            if i + 1 < count and term[i + 1] is not None:
                pieces.append(betas[i] * term[i + 1])
            if i > 0 and term[i - 1] is not None:
                pieces.append(betas[i - 1] * term[i - 1])
            fresh.append(sum(pieces[1:], pieces[0]) * (time_step / order) if pieces else None)
        term = fresh
        into = imag if order % 2 else real
        minus = order % 4 in (1, 2)
        for i in range(count):
            if term[i] is not None:
                if into[i] is None:
                    into[i] = -term[i] if minus else term[i]
                else:
                    into[i] = into[i] - term[i] if minus else into[i] + term[i]
    zero = jnp.zeros((SUB, LANES), jnp.float32)
    return [zero if r is None else r for r in real], [zero if m is None else m for m in imag]


def kernel(n, nx, nz, psi_ref, pot_ref, out_ref, send, recv, basis, outb, back, pots, mix,
           send_sem, recv_sem, pot_send, pot_recv, back_send, back_recv):
    me = lax.axis_index("dom")
    mesh_ids = pl.DeviceIdType.MESH
    barrier = pltpu.get_barrier_semaphore()

    def greet(k, carry):
        pl.semaphore_signal(barrier, inc=1, device_id={"dom": lax.rem(me + k, n)}, device_id_type=mesh_ids)
        return carry

    lax.fori_loop(1, n, greet, 0)

    def forward(c, here, there):
        return pltpu.make_async_remote_copy(
            src_ref=send.at[c, there], dst_ref=recv.at[c, here + 1],
            send_sem=send_sem.at[c, there], recv_sem=recv_sem.at[c, here],
            device_id={"dom": there}, device_id_type=mesh_ids)

    def pot_copy(here, there):
        return pltpu.make_async_remote_copy(
            src_ref=pot_ref, dst_ref=pots.at[here],
            send_sem=pot_send.at[there], recv_sem=pot_recv.at[here],
            device_id={"dom": there}, device_id_type=mesh_ids)

    def backward(c, here, there):
        return pltpu.make_async_remote_copy(
            src_ref=outb.at[c, there], dst_ref=back.at[c, here],
            send_sem=back_send.at[c, there], recv_sem=back_recv.at[c, here],
            device_id={"dom": there}, device_id_type=mesh_ids)

    low = lax.broadcasted_iota(jnp.int32, (n, SUB, LANES), 1) < HALF

    def interleave(a, b):
        return (jnp.where(low, a, pltpu.roll(b, HALF, 1)), jnp.where(low, pltpu.roll(a, HALF, 1), b))

    def pack(x, carry):
        parts = [psi_ref[p * nx + x].T.reshape(n, SUB, LANES) for p in range(2)]
        for c, block in enumerate(interleave(*parts)):
            send[c, :, x] = block
        return carry

    lax.fori_loop(0, nx, pack, 0)

    pots[me] = pot_ref[...]
    blank = jnp.zeros((nx, SUB, LANES), jnp.float32)
    for c in range(CHUNKS):
        recv[c, me + 1] = send[c, me]
        recv[c, 0] = blank
        recv[c, n + 1] = blank
    for j in range(ITERS - 1):
        basis[j, 0] = blank
        basis[j, n + 1] = blank

    pl.semaphore_wait(barrier, n - 1)

    def send_pot(k, carry):
        pot_copy(me, lax.rem(me + k, n)).start()
        return carry

    lax.fori_loop(1, n, send_pot, 0)
    for c in range(CHUNKS):
        def send_one(k, carry, c=c):
            forward(c, me, lax.rem(me + k, n)).start()
            return carry

        lax.fori_loop(1, n, send_one, 0)

    def wait_pot(k, carry):
        there = lax.rem(me + n - k, n)
        pot_copy(there, there).wait_recv()
        return carry

    upper = lax.broadcasted_iota(jnp.int32, (SUB, LANES), 1) >= nz
    sign = jnp.where(lax.broadcasted_iota(jnp.int32, (SUB, LANES), 0) < HALF, 1.0, -1.0)
    ratio = -0.5 * far_weight

    row = lax.broadcasted_iota(jnp.int32, (LANES, LANES), 0)
    column = lax.broadcasted_iota(jnp.int32, (LANES, LANES), 1)
    apart = lax.rem(row - column + 2 * nz, nz)
    near_z = jnp.where(jnp.logical_or(apart == 1, apart == nz - 1), 16.0, 0.0)
    far_z = jnp.where(jnp.logical_or(apart == 2, apart == nz - 2), 1.0, 0.0)
    same = (row < nz) == (column < nz)
    lanes_matrix = jnp.where(same, far_z - near_z, jnp.where(apart == 0, -16.0, 0.0)).astype(jnp.bfloat16)
    mix[0:LANES] = lanes_matrix
    mix[LANES:2 * LANES] = lanes_matrix

    def applied_at(ref, s):
        slabs = [[ref[s + g, x] for x in range(nx)] for g in range(GROUP + 2)]
        inner = jnp.concatenate([u for slab in slabs[1:-1] for u in slab], axis=0)
        high = inner.astype(jnp.bfloat16)
        rest = (inner - high.astype(jnp.float32)).astype(jnp.bfloat16)
        mixed = jnp.dot(jnp.concatenate([high, rest], axis=1), mix[...], preferred_element_type=jnp.float32)
        result = []
        for g in range(GROUP):
            before, now, after = slabs[g:g + 3]
            for x in range(nx):
                u = now[x]
                close = now[(x + 1) % nx] + now[(x - 1) % nx]
                close = close + pltpu.roll(jnp.where(upper, before[x], after[x]), nz, 1)
                wide = now[(x + 2) % nx] + now[(x - 2) % nx] + before[x] + after[x]
                at = (g * nx + x) * SUB
                wide = wide + mixed[at:at + SUB]
                own = jnp.broadcast_to(pots[s + g, pl.ds(x, 1), :], (SUB, LANES)) + -0.5 * centre_weight
                result.append((own * u + ratio * (wide - 16.0 * close), u))
        return result

    def chunk(c, carry):
        vectors = [recv.at[c]] + [basis.at[j] for j in range(ITERS - 1)]

        def arrive(k, acc):
            there = lax.rem(me + n - k, n)
            forward(c, there, there).wait_recv()
            for x in range(nx):
                u = recv[c, there + 1, x]
                acc = acc + u * u
            return acc

        acc = jnp.zeros((SUB, LANES), jnp.float32)
        for x in range(nx):
            u = recv[c, me + 1, x]
            acc = acc + u * u
        acc = lax.fori_loop(1, n, arrive, acc)
        first_norm = jnp.sqrt(total_of(acc) + epsilon)

        @pl.when(c == 0)
        def _():
            lax.fori_loop(1, n, wait_pot, 0)

        scales = [1.0 / first_norm]
        alphas, betas = [], []
        zero = jnp.zeros((SUB, LANES), jnp.float32)
        for j in range(ITERS):
            ref = vectors[j]
            last = j + 1 == ITERS
            fresh = None if last else vectors[j + 1]

            def apply(s, accs, ref=ref, fresh=fresh):
                accs = list(accs)
                for at, (w, u) in enumerate(applied_at(ref, s * GROUP)):
                    if fresh is not None:
                        fresh[s * GROUP + at // nx + 1, at % nx] = w
                    accs[at % 2] = accs[at % 2] + u * w
                return tuple(accs)

            accs = lax.fori_loop(0, n // GROUP, apply, (zero, zero), unroll=UNROLL_A)
            scale = scales[j]
            alpha = scale * (scale * total_of(accs[0] + accs[1]))
            alphas.append(alpha)
            if last:
                break
            by_self = alpha * scale
            by_previous = betas[j - 1] * scales[j - 1] if j else None

            def reduce(s, accs, ref=ref, fresh=fresh, scale=scale, by_self=by_self, by_previous=by_previous, j=j):
                accs = list(accs)
                for x in range(nx):
                    r = scale * fresh[s + 1, x] - by_self * ref[s + 1, x]
                    if j:
                        r = r - by_previous * vectors[j - 1][s + 1, x]
                    fresh[s + 1, x] = r
                    accs[x % 2] = accs[x % 2] + r * r
                return tuple(accs)

            accs = lax.fori_loop(0, n, reduce, (zero, zero), unroll=UNROLL_B)
            beta = jnp.sqrt(total_of(accs[0] + accs[1]) + epsilon)
            betas.append(beta)
            scales.append(1.0 / beta)

        real, imag = krylov_weights(alphas, betas)
        straight = [first_norm * scales[j] * real[j] for j in range(ITERS)]
        crossed = [first_norm * scales[j] * imag[j] * sign for j in range(ITERS)]

        def combined(d, x):
            us = [v[d + 1, x] for v in vectors]
            a = straight[0] * us[0]
            b = crossed[0] * us[0]
            for j in range(1, ITERS):
                a = a + straight[j] * us[j]
                b = b + crossed[j] * us[j]
            return a + swap_parts(b)

        def finish(k, carry):
            there = lax.rem(me + k, n)
            for x in range(nx):
                outb[c, there, x] = combined(there, x)

            @pl.when(k > 1)
            def _():
                backward(c, me, lax.rem(me + k - 1, n)).start()

            return carry

        lax.fori_loop(1, n, finish, 0)
        for x in range(nx):
            back[c, me, x] = combined(me, x)
        backward(c, me, lax.rem(me + n - 1, n)).start()
        return carry

    lax.fori_loop(0, CHUNKS, chunk, 0)

    for c in range(CHUNKS):
        def returned(k, carry, c=c):
            there = lax.rem(me + n - k, n)
            backward(c, there, there).wait_recv()
            return carry

        lax.fori_loop(1, n, returned, 0)

    def unpack(x, carry):
        for p, block in enumerate(interleave(back[0, :, x], back[1, :, x])):
            out_ref[p * nx + x] = block.reshape(n * SUB, LANES).T
        return carry

    lax.fori_loop(0, nx, unpack, 0)

    def sent(k, carry):
        there = lax.rem(me + k, n)
        pot_copy(me, there).wait_send()
        for c in range(CHUNKS):
            forward(c, me, there).wait_send()
            backward(c, me, there).wait_send()
        return carry

    lax.fori_loop(1, n, sent, 0)


def fused(psi, potential, n):
    parts, slabs, nx, by, nz, orbs = psi.shape
    rows = nx * by * nz // LANES
    vec = lambda *lead: pltpu.VMEM(lead + (nx, SUB, LANES), jnp.float32)
    dma = lambda *shape: pltpu.SemaphoreType.DMA(shape)
    result = pl.pallas_call(
        functools.partial(kernel, n, nx, nz),
        out_shape=jax.ShapeDtypeStruct((parts * nx, by * nz, orbs), jnp.float32),
        in_specs=[pl.BlockSpec(memory_space=pltpu.VMEM)] * 2,
        out_specs=pl.BlockSpec(memory_space=pltpu.VMEM),
        scratch_shapes=[
            vec(CHUNKS, n), vec(CHUNKS, n + 2), vec(ITERS - 1, n + 2), vec(CHUNKS, n), vec(CHUNKS, n),
            pltpu.VMEM((n, nx, LANES), jnp.float32), pltpu.VMEM((2 * LANES, LANES), jnp.bfloat16),
            dma(CHUNKS, n), dma(CHUNKS, n), dma(n), dma(n), dma(CHUNKS, n), dma(CHUNKS, n),
        ],
        compiler_params=pltpu.CompilerParams(collective_id=0, has_side_effects=True),
    )(psi.reshape(parts * nx, by * nz, orbs), potential.reshape(nx, by * nz))
    return result.reshape(psi.shape)


def fits(psi, n):
    parts, slabs, nx, by, nz, orbs = psi.shape
    return parts == 2 and slabs == 1 and by == 2 and by * nz == LANES and orbs == LANES and orbs == n * SUB and n % GROUP == 0


def per_device(n, psi, potential):
    if fits(psi, n):
        return fused(psi, potential, n)
    return on_device(psi, potential)


def solution(mesh):
    placed = (P(None, "dom", None, None, None, "st"), P("dom", None, None, None))
    return jax.shard_map(
        functools.partial(per_device, mesh.shape["dom"]),
        mesh=mesh,
        in_specs=placed,
        out_specs=P(None, "dom", None, None, None, "st"),
        check_vma=False,
    )
```
